32 devices in a mesh: patch: 8 (over y, x, core), tensor: 4 (over z).
Axes of the slice: x: 2, y: 2, z: 4, core: 2. Of those that a mesh axis runs over, the one named last changes fastest.
Arguments:
- tokens: bfloat16 [8192, 3072], P(('patch', 'tensor')), may hold values from -6 to 6
- text_tokens: bfloat16 [512, 3072], P('patch'), may hold values from -6 to 6
- img_shift: float32 [3072], replicated, may hold values from -3 to 3
- img_scale: float32 [3072], replicated, may hold values from -3 to 3
- img_gate: float32 [3072], replicated, may hold values from 0.5 to 2
- txt_shift: float32 [3072], replicated, may hold values from -3 to 3
- txt_scale: float32 [3072], replicated, may hold values from -3 to 3
- qkv_weight: bfloat16 [3072, 3, 2048], P(None, None, 'tensor'), may hold values from -0.109375 to 0.109375
- txt_kv_weight: bfloat16 [3072, 2, 2048], P(None, None, 'tensor'), may hold values from -0.109375 to 0.109375
- q_gain: float32 [128], replicated, may hold values from 1 to 3
- k_gain: float32 [128], replicated, may hold values from 1 to 3
- txt_k_gain: float32 [128], replicated, may hold values from 1 to 3
- out_weight: bfloat16 [2048, 3072], P('tensor'), may hold values from -0.125 to 0.125
- stale_keys: bfloat16 [8192, 2048], P('patch', 'tensor'), may hold values from -600 to 600
- stale_values: bfloat16 [8192, 2048], P('patch', 'tensor'), may hold values from -6 to 6
Outputs:
- updated: bfloat16 [8192, 3072], P(('patch', 'tensor'))
- new_keys: bfloat16 [8192, 2048], P('patch', 'tensor')
- new_values: bfloat16 [8192, 2048], P('patch', 'tensor')
The draws below stay inside these ranges and needn't reach their ends.
All inputs are finite; a program needn't handle non-finite values.
Results may differ from the reference program's by a relative error of at most 0.015.
The reference program's roundings to bfloat16 on the way (of `image_mod`, `text_mod` and `attended`) count: a program that leaves them out, or rounds other values in their place, can miss the bound.
Values may be sent and summed in bfloat16 or wider, within the bound.
A program may use at most 320 MiB of HBM per device.

```python
import math
import jax
import jax.numpy as jnp
from jax import lax

D = 3072
HD = 128
HEADS = 16
ROWS = 1024
TXT = 512
IMG = 8192
N_PATCH = 8


def draw_stale_keys(key, part):
    first = jax.random.fold_in(key, 0)
    base = jnp.clip(2.0 * jax.random.normal(first, (IMG, HEADS * HD), jnp.float32), -12.0, 12.0)
    return base.astype(jnp.bfloat16)


def block_levels(rng, dims, shards, smallest, high):
    def one(dim, blocks):
        steps = jax.random.uniform(jax.random.fold_in(jax.random.fold_in(rng, 6), dim), (blocks,), jnp.float32, smallest / len(shards), high / len(shards))
        return jnp.repeat(jnp.exp(steps), dims[dim] // blocks).reshape((-1,) + (1,) * (len(dims) - dim - 1))

    loudness = one(*shards[0])
    for cut in shards[1:]:
        loudness = loudness * one(*cut)
    return loudness


def scatter_about(rng, shape, deviation, reach, cuts=(), kind=jnp.bfloat16):
    level = block_levels(rng, shape, cuts, -0.22, 0.18) if cuts else 1.0
    result = jax.random.normal(rng, shape, jnp.float32) * deviation * level
    return jnp.minimum(jnp.maximum(result, -reach), reach).astype(kind)


def setup_inputs(seed: int = 0) -> dict:
    keys = jax.random.split(jax.random.key(seed), 16)
    tokens = scatter_about(keys[0], (IMG, D), 1.0, 6.0, ((0, 32),))
    text_tokens = scatter_about(keys[1], (TXT, D), 1.0, 6.0, ((0, 8),))
    img_shift = scatter_about(keys[2], (D,), 0.5, 3.0, (), jnp.float32)
    img_scale = scatter_about(keys[3], (D,), 0.5, 3.0, (), jnp.float32)
    img_gate = jnp.clip(jax.random.uniform(keys[4], (D,), jnp.float32, 0.5, 2.0), 0.5, 2.0)
    txt_shift = scatter_about(keys[5], (D,), 0.5, 3.0, (), jnp.float32)
    txt_scale = scatter_about(keys[6], (D,), 0.5, 3.0, (), jnp.float32)
    qkv_weight = scatter_about(keys[7], (D, 3, HEADS * HD), D ** -0.5, 0.109375, ((2, 4),))
    txt_kv_weight = scatter_about(keys[8], (D, 2, HEADS * HD), D ** -0.5, 0.109375, ((2, 4),))
    q_gain = jnp.clip(jnp.exp(jax.random.uniform(keys[9], (HD,), jnp.float32, math.log(1.0), math.log(3.0))), 1.0, 3.0)
    k_gain = jnp.clip(jnp.exp(jax.random.uniform(keys[10], (HD,), jnp.float32, math.log(1.0), math.log(3.0))), 1.0, 3.0)
    txt_k_gain = jnp.clip(jnp.exp(jax.random.uniform(keys[11], (HD,), jnp.float32, math.log(1.0), math.log(3.0))), 1.0, 3.0)
    out_weight = scatter_about(keys[12], (HEADS * HD, D), (HEADS * HD) ** -0.5, 0.125, ((0, 4),))
    stale_keys = draw_stale_keys(jax.random.fold_in(keys[15], 71), 0)
    stale_values = scatter_about(keys[14], (IMG, HEADS * HD), 1.0, 6.0, ((0, 8), (1, 4)))
    return dict(tokens=tokens, text_tokens=text_tokens, img_shift=img_shift, img_scale=img_scale, img_gate=img_gate, txt_shift=txt_shift, txt_scale=txt_scale, qkv_weight=qkv_weight, txt_kv_weight=txt_kv_weight, q_gain=q_gain, k_gain=k_gain, txt_k_gain=txt_k_gain, out_weight=out_weight, stale_keys=stale_keys, stale_values=stale_values)


def layer_mod(values, shift_vec, scale_vec):
    wide = values.astype(jnp.float32)
    centre = lax.optimization_barrier(jnp.mean(wide, axis=-1, keepdims=True))
    spread = lax.optimization_barrier(jnp.mean((wide - centre) * (wide - centre), axis=-1, keepdims=True))
    normed = (wide - centre) * lax.rsqrt(spread + 1e-06)
    return ((1.0 + scale_vec) * normed + shift_vec).astype(jnp.bfloat16)

def rms_gain(values, gain_vec):
    square = lax.optimization_barrier(jnp.mean(values * values, axis=-1, keepdims=True))
    return values * lax.rsqrt(square + 1e-06) * gain_vec

def reference(tokens, text_tokens, img_shift, img_scale, img_gate, txt_shift, txt_scale, qkv_weight, txt_kv_weight, q_gain, k_gain, txt_k_gain, out_weight, stale_keys, stale_values):
    image_mod = layer_mod(tokens, img_shift, img_scale)
    projected = jnp.dot(image_mod, qkv_weight.reshape(D, 3 * HEADS * HD), preferred_element_type=jnp.float32)
    projected = projected.reshape(IMG, 3, HEADS, HD)
    queries = rms_gain(projected[:, 0], q_gain).astype(jnp.bfloat16)
    fresh_keys = rms_gain(projected[:, 1], k_gain).astype(jnp.bfloat16)
    fresh_values = projected[:, 2].astype(jnp.bfloat16)
    text_mod = layer_mod(text_tokens, txt_shift, txt_scale)
    text_proj = jnp.dot(text_mod, txt_kv_weight.reshape(D, 2 * HEADS * HD), preferred_element_type=jnp.float32)
    text_proj = text_proj.reshape(TXT, 2, HEADS, HD)
    text_keys = rms_gain(text_proj[:, 0], txt_k_gain).astype(jnp.bfloat16)
    text_values = text_proj[:, 1].astype(jnp.bfloat16)
    old_keys = stale_keys.reshape(IMG, HEADS, HD)
    old_values = stale_values.reshape(IMG, HEADS, HD)
    factor = 1.0 / math_sqrt(HD)
    zero = jnp.int32(0)

    def one_patch(patch_idx):
        offset = (patch_idx * ROWS).astype(jnp.int32)
        own_keys = lax.dynamic_slice_in_dim(fresh_keys, offset, ROWS, 0)
        own_values = lax.dynamic_slice_in_dim(fresh_values, offset, ROWS, 0)
        key_rows = lax.dynamic_update_slice(old_keys, own_keys, (offset, zero, zero))
        value_rows = lax.dynamic_update_slice(old_values, own_values, (offset, zero, zero))
        key_rows = jnp.concatenate([key_rows, text_keys], axis=0)
        value_rows = jnp.concatenate([value_rows, text_values], axis=0)
        query_rows = lax.dynamic_slice_in_dim(queries, offset, ROWS, 0)
        scores = jnp.einsum('qhd,khd->hqk', query_rows.astype(jnp.float32), key_rows.astype(jnp.float32)) * factor
        highest = lax.optimization_barrier(jnp.max(scores, axis=-1, keepdims=True))
        weights = jnp.exp(scores - highest)
        denominator = lax.optimization_barrier(jnp.sum(weights, axis=-1))
        rounded = weights.astype(jnp.bfloat16).astype(jnp.float32)
        numerator = jnp.einsum('hqk,khd->qhd', rounded, value_rows.astype(jnp.float32))
        return (numerator / jnp.transpose(denominator)[:, :, None]).astype(jnp.bfloat16)
    attended = lax.map(one_patch, jnp.arange(N_PATCH, dtype=jnp.int32)).reshape(IMG, HEADS * HD)
    branch = jnp.dot(attended, out_weight, preferred_element_type=jnp.float32)
    updated = (tokens.astype(jnp.float32) + img_gate * branch).astype(jnp.bfloat16)
    return (updated, fresh_keys.reshape(IMG, HEADS * HD), fresh_values.reshape(IMG, HEADS * HD))

def math_sqrt(number):
    return float(number) ** 0.5
```

```python
import functools
import math

import jax
import jax.numpy as jnp
from jax import lax
from jax.experimental import pallas as pl
from jax.experimental.pallas import tpu as pltpu
from jax.sharding import PartitionSpec as P


def layer_mod(values, shift_vec, scale_vec):
    wide = values.astype(jnp.float32)
    centre = jnp.mean(wide, axis=-1, keepdims=True)
    spread = jnp.mean((wide - centre) * (wide - centre), axis=-1, keepdims=True)
    normed = (wide - centre) * lax.rsqrt(spread + 1e-06)
    return ((1.0 + scale_vec) * normed + shift_vec).astype(jnp.bfloat16)


def project_kernel(head_dim, x_ref, w_ref, g_ref, o_ref):
    part = pl.program_id(0)
    plain = part == pl.num_programs(0) - 1
    prod = jnp.dot(x_ref[...], w_ref[0], preferred_element_type=jnp.float32)
    gain = g_ref[0]
    for h in range(prod.shape[1] // head_dim):
        cols = slice(h * head_dim, (h + 1) * head_dim)
        piece = prod[:, cols]
        square = jnp.mean(piece * piece, axis=-1, keepdims=True)
        normed = piece * lax.rsqrt(square + 1e-06) * gain
        o_ref[0, :, cols] = jnp.where(plain, piece, normed).astype(jnp.bfloat16)


def project(x, weight, gains, head_dim):
    rows, width = x.shape
    parts, _, cols = weight.shape
    tile = min(rows, 512)
    return pl.pallas_call(
        functools.partial(project_kernel, head_dim),
        grid=(parts, rows // tile),
        out_shape=jax.ShapeDtypeStruct((parts, rows, cols), jnp.bfloat16),
        in_specs=[
            pl.BlockSpec((tile, width), lambda j, i: (i, 0)),
            pl.BlockSpec((1, width, cols), lambda j, i: (j, 0, 0)),
            pl.BlockSpec((1, 1, head_dim), lambda j, i: (j, 0, 0)),
        ],
        out_specs=pl.BlockSpec((1, tile, cols), lambda j, i: (j, i, 0)),
        cost_estimate=pl.CostEstimate(
            flops=2 * rows * width * cols * parts,
            bytes_accessed=2 * (parts * width * cols + parts * rows * (width + cols)),
            transcendentals=0,
        ),
    )(x, weight, gains)


def attend_kernel(scale, chunk, q_ref, ks_ref, vs_ref, kf_ref, vf_ref, kt_ref, vt_ref, o_ref):
    q = q_ref[...]
    rows, head_dim = q.shape
    blocks = []
    for k_ref, v_ref in ((ks_ref, vs_ref), (kf_ref, vf_ref), (kt_ref, vt_ref)):
        total = k_ref.shape[0]
        step = min(total, chunk)
        for start in range(0, total, step):
            blocks.append((k_ref, v_ref, start, step))

    def score(block):
        k_ref, _, start, step = block
        return lax.dot_general(
            q, k_ref[pl.ds(start, step), :], (((1,), (1,)), ((), ())),
            preferred_element_type=jnp.float32,
        )

    peak = jnp.full((rows, 1), -1e30, jnp.float32)
    denom = jnp.zeros((rows, 128), jnp.float32)
    numer = jnp.zeros((rows, head_dim), jnp.float32)
    ahead = score(blocks[0])
    for idx, block in enumerate(blocks):
        scores = ahead
        if idx + 1 < len(blocks):
            ahead = score(blocks[idx + 1])
        _, v_ref, start, step = block
        new_peak = jnp.maximum(peak, jnp.max(scores, axis=-1, keepdims=True))
        rescale = jnp.exp2((peak - new_peak) * scale)
        weights = jnp.exp2((scores - new_peak) * scale)
        part = weights[:, :128]
        for lane in range(128, step, 128):
            part = part + weights[:, lane : lane + 128]
        denom = denom * rescale + part
        numer = numer * rescale + jnp.dot(
            weights.astype(jnp.bfloat16), v_ref[pl.ds(start, step), :],
            preferred_element_type=jnp.float32,
        )
        peak = new_peak
    o_ref[...] = (numer / jnp.sum(denom, axis=-1, keepdims=True)).astype(jnp.bfloat16)


def attend(q, stale, fresh, text, head_dim):
    rows, cols = q.shape
    heads = cols // head_dim
    tile = min(rows, 256)
    scale = math.log2(math.e) / float(head_dim) ** 0.5

    def keyed(arr):
        return pl.BlockSpec((arr.shape[0], head_dim), lambda h, i: (0, h))

    pairs = [*stale, *fresh, *text]
    n_keys = stale[0].shape[0] + fresh[0].shape[0] + text[0].shape[0]
    return pl.pallas_call(
        functools.partial(attend_kernel, scale, 1024),
        grid=(heads, rows // tile),
        out_shape=jax.ShapeDtypeStruct((rows, cols), jnp.bfloat16),
        in_specs=[pl.BlockSpec((tile, head_dim), lambda h, i: (i, h))] + [keyed(a) for a in pairs],
        out_specs=pl.BlockSpec((tile, head_dim), lambda h, i: (i, h)),
        cost_estimate=pl.CostEstimate(
            flops=4 * rows * n_keys * cols * 2,
            bytes_accessed=4 * (rows + n_keys) * cols,
            transcendentals=rows * n_keys * heads,
        ),
    )(q, *pairs)


def after(blocks, gate):
    names = list(blocks)
    tied = lax.optimization_barrier(tuple(blocks[m] for m in names) + (gate,))
    return dict(zip(names, tied))


def finish_kernel(n_patch, x_ref, t_ref, g_ref, *refs):
    own = lax.axis_index("patch")
    o_ref = refs[n_patch]
    total = jnp.zeros(o_ref.shape, jnp.float32)
    for m in range(n_patch):
        owner = lax.bitwise_xor(own, m)
        total = total + jnp.dot(x_ref[owner], refs[m][...], preferred_element_type=jnp.float32)
    o_ref[...] = (t_ref[...].astype(jnp.float32) + g_ref[...] * total).astype(jnp.bfloat16)


def finish(spread, tokens, gate, blocks):
    n_patch, rows, depth = spread.shape
    width = tokens.shape[1]
    tile = 512 if width % 512 == 0 else width
    return pl.pallas_call(
        functools.partial(finish_kernel, n_patch),
        grid=(width // tile,),
        out_shape=jax.ShapeDtypeStruct(tokens.shape, jnp.bfloat16),
        in_specs=[
            pl.BlockSpec((n_patch, rows, depth), lambda j: (0, 0, 0)),
            pl.BlockSpec((rows, tile), lambda j: (0, j)),
            pl.BlockSpec((1, tile), lambda j: (0, j)),
        ]
        + [pl.BlockSpec((depth, tile), lambda j: (0, j))] * n_patch,
        out_specs=pl.BlockSpec((rows, tile), lambda j: (0, j)),
        cost_estimate=pl.CostEstimate(
            flops=2 * rows * width * depth * n_patch,
            bytes_accessed=2 * n_patch * depth * (rows + width),
            transcendentals=0,
        ),
    )(spread, tokens, gate[None, :], *blocks)


def patch_blocks(x, n, order, held=None):
    held = {0: x} if held is None else held
    for bit in order:
        flip = 1 << bit
        pairs = [(i, i ^ flip) for i in range(n)]
        moved = {m ^ flip: lax.ppermute(a, "patch", pairs) for m, a in held.items()}
        held.update(moved)
    return held


def per_device(
    n_patch,
    n_tensor,
    tokens,
    text_tokens,
    img_shift,
    img_scale,
    img_gate,
    txt_shift,
    txt_scale,
    qkv_weight,
    txt_kv_weight,
    q_gain,
    k_gain,
    txt_k_gain,
    out_weight,
    stale_keys,
    stale_values,
):
    width = tokens.shape[1]
    head_dim = q_gain.shape[0]
    cols = qkv_weight.shape[2]
    own = lax.axis_index("patch")
    slot = lax.axis_index("tensor")
    bits = n_patch.bit_length() - 1
    far = list(range(1, bits))
    one_way = far + [0]
    other_way = far[::-1] + [0]

    key_blocks = patch_blocks(stale_keys, n_patch, one_way)
    value_blocks = patch_blocks(stale_values, n_patch, other_way)

    image_mod = layer_mod(tokens, img_shift, img_scale)
    patch_mod = lax.all_gather(image_mod, "tensor", axis=0, tiled=True)

    text_mod = layer_mod(text_tokens, txt_shift, txt_scale)
    ones = jnp.ones_like(k_gain)
    text_own = project(
        text_mod,
        jnp.transpose(txt_kv_weight, (1, 0, 2)),
        jnp.stack([txt_k_gain, ones])[:, None, :],
        head_dim,
    )
    text_blocks = patch_blocks(text_own, n_patch, one_way)
    text_all = jnp.concatenate([text_blocks[m] for m in range(n_patch)], axis=1)

    share = out_weight.shape[0] // n_patch
    mine = lax.dynamic_slice_in_dim(out_weight, own * share, share, 0)
    shares = jnp.zeros((n_tensor, share, width), out_weight.dtype)
    for shift in range(n_tensor):
        if shift == 0:
            piece = mine
        else:
            ring = [(i, (i + shift) % n_tensor) for i in range(n_tensor)]
            piece = lax.ppermute(mine, "tensor", ring)
        owner = lax.rem(slot + n_tensor - shift, n_tensor)
        shares = lax.dynamic_update_slice(shares, piece[None], (owner, 0, 0))
    shares = shares.reshape(n_tensor * share, width)
    share_blocks = patch_blocks(shares, n_patch, other_way[:1])

    stale_k = jnp.concatenate([key_blocks[m] for m in range(1, n_patch)], axis=0)
    stale_v = jnp.concatenate([value_blocks[m] for m in range(1, n_patch)], axis=0)

    qkv = project(
        patch_mod,
        jnp.transpose(qkv_weight, (1, 0, 2)),
        jnp.stack([q_gain, k_gain, ones])[:, None, :],
        head_dim,
    )
    queries, fresh_keys, fresh_values = qkv[0], qkv[1], qkv[2]
    share_blocks = after(share_blocks, queries)
    share_blocks = patch_blocks(None, n_patch, other_way[1:-1], share_blocks)

    rows = tokens.shape[0]
    spread = jnp.zeros((rows, n_tensor * cols), jnp.bfloat16)
    parts = []
    for shift in [*range(1, n_tensor), 0]:
        owner = lax.rem(slot + shift, n_tensor)
        part = attend(
            lax.dynamic_slice_in_dim(queries, owner * rows, rows, 0),
            (stale_k, stale_v),
            (fresh_keys, fresh_values),
            (text_all[0], text_all[1]),
            head_dim,
        )
        parts.append(part)
        if shift:
            ring = [(i, (i + shift) % n_tensor) for i in range(n_tensor)]
            part = lax.ppermute(part, "tensor", ring)
        source = lax.rem(slot + n_tensor - shift, n_tensor)
        spread = lax.dynamic_update_slice(spread, part, (0, source * cols))
    share_blocks = after(share_blocks, parts[-2])
    share_blocks = patch_blocks(None, n_patch, other_way[-1:], share_blocks)
    spread = spread.reshape(rows, n_tensor, n_patch, share)
    spread = jnp.transpose(spread, (2, 0, 1, 3)).reshape(n_patch, rows, n_tensor * share)
    updated = finish(spread, tokens, img_gate, [share_blocks[m] for m in range(n_patch)])
    return (updated, fresh_keys, fresh_values)


def solution(mesh):
    placed = (
        P(("patch", "tensor"), None),
        P("patch", None),
        P(),
        P(),
        P(),
        P(),
        P(),
        P(None, None, "tensor"),
        P(None, None, "tensor"),
        P(),
        P(),
        P(),
        P("tensor", None),
        P("patch", "tensor"),
        P("patch", "tensor"),
    )
    return jax.shard_map(
        functools.partial(per_device, mesh.shape["patch"], mesh.shape["tensor"]),
        mesh=mesh,
        in_specs=placed,
        out_specs=(P(("patch", "tensor"), None), P("patch", "tensor"), P("patch", "tensor")),
        check_vma=False,
    )
```
